32 devices in a mesh: dp: 1 (over z), tp: 4 (over y), cp: 8 (over x, core).
Axes of the slice: x: 4, y: 4, z: 1, core: 2. Of those that a mesh axis runs over, the one named last changes fastest.
The devices are a block of a 4x4x8 slice.
Arguments:
- x: bfloat16 [8192, 5120], P(('dp', 'cp', 'tp'))
- pos: int32 [8192], P(('dp', 'cp', 'tp'))
- g1: bfloat16 [5120], replicated
- g2: bfloat16 [5120], replicated
- wq: bfloat16 [5120, 5120], P(None, 'tp')
- wk: bfloat16 [5120, 1024], P(None, 'tp')
- wv: bfloat16 [5120, 1024], P(None, 'tp')
- wo: bfloat16 [5120, 5120], P('tp')
- w1: bfloat16 [5120, 13824], P(None, 'tp')
- w3: bfloat16 [5120, 13824], P(None, 'tp')
- w2: bfloat16 [13824, 5120], P('tp')
Outputs:
- output: bfloat16 [8192, 5120], P(('dp', 'cp', 'tp'))
All inputs are finite; a program needn't handle non-finite values.
Results may differ from the reference program's by a relative error of at most 0.00970005.
Values are sent between devices in bfloat16 or wider.
A program may use at most 768 MiB of HBM per device.

```python
import math
import jax
import jax.numpy as jnp
from jax import lax

T = 8192
D = 5120
HQ = 40
HKV = 8
DH = 128
F = 13824
NDEV = 32
QB = 64
PIECE = T // (2 * NDEV)
GRP = HQ // HKV
EPS = 1e-5
THETA = 500000.0


def setup_inputs(seed: int = 0, part: int = 0) -> dict:
    kpart = jax.random.fold_in(jax.random.key(seed), part)
    kx, kgap, kstart = jax.random.split(kpart, 3)
    kw = jax.random.split(jax.random.key(seed + 1), 9)
    x = jax.random.normal(kx, (T, D), jnp.float32).astype(jnp.bfloat16)
    gaps = jax.random.randint(kgap, (T,), 1, 4)
    start = jax.random.randint(kstart, (), 0, T)
    seqpos = start + jnp.cumsum(gaps) - gaps[0]
    rows = jnp.arange(T)
    dev = rows // (2 * PIECE)
    off = rows % (2 * PIECE)
    piece = jnp.where(off < PIECE, dev, 2 * NDEV - 1 - dev)
    pos = seqpos[piece * PIECE + off % PIECE].astype(jnp.int32)
    qk = math.sqrt(math.sqrt(math.log(T / 16.0)))

    def nrm(k, shape, scl):
        return (jax.random.normal(k, shape, jnp.float32) * scl).astype(jnp.bfloat16)

    g1 = (1.0 + 0.3 * jax.random.normal(kw[0], (D,), jnp.float32)).astype(jnp.bfloat16)
    g2 = (1.0 + 0.3 * jax.random.normal(kw[1], (D,), jnp.float32)).astype(jnp.bfloat16)
    wq = nrm(kw[2], (D, HQ * DH), qk / math.sqrt(D))
    wk = nrm(kw[3], (D, HKV * DH), qk / math.sqrt(D))
    wv = nrm(kw[4], (D, HKV * DH), 1.0 / math.sqrt(D))
    wo = nrm(kw[5], (HQ * DH, D), 2.0 / math.sqrt(HQ * DH))
    w1 = nrm(kw[6], (D, F), 1.0 / math.sqrt(D))
    w3 = nrm(kw[7], (D, F), 1.0 / math.sqrt(D))
    w2 = nrm(kw[8], (F, D), 1.0 / math.sqrt(F))
    return dict(x=x, pos=pos, g1=g1, g2=g2, wq=wq, wk=wk, wv=wv, wo=wo, w1=w1, w3=w3, w2=w2)


def rms_norm(v, g):
    vf = v.astype(jnp.float32)
    inv = lax.rsqrt(jnp.mean(vf * vf, axis=-1, keepdims=True) + EPS)
    return (vf * inv * g.astype(jnp.float32)).astype(jnp.bfloat16)


def rope(y, p):
    half = DH // 2
    freq = 1.0 / (THETA ** (jnp.arange(0, DH, 2, dtype=jnp.float32) / DH))
    ang = p.astype(jnp.float32)[..., None] * freq
    c = jnp.cos(ang)[..., None, :]
    s = jnp.sin(ang)[..., None, :]
    y1 = y[..., :half]
    y2 = y[..., half:]
    return jnp.concatenate([y1 * c - y2 * s, y2 * c + y1 * s], axis=-1)


def attention(q, k, v, p):
    qr = q.reshape(T // QB, QB, HKV, GRP, DH)
    pr = p.reshape(T // QB, QB)
    kf = k.astype(jnp.float32)
    vf = v.astype(jnp.float32)
    scale = 1.0 / math.sqrt(DH)

    def blk(qp):
        qq, pp = qp
        s = jnp.einsum('qkgd,skd->kgqs', qq.astype(jnp.float32), kf) * scale
        s = jnp.where(p[None, None, None, :] <= pp[None, None, :, None], s, -1e30)
        e = jnp.exp(s - jnp.max(s, axis=-1, keepdims=True))
        w = (e / jnp.sum(e, axis=-1, keepdims=True)).astype(jnp.bfloat16)
        o = jnp.einsum('kgqs,skd->qkgd', w.astype(jnp.float32), vf)
        return o.astype(jnp.bfloat16)

    return lax.map(blk, (qr, pr)).reshape(T, HQ * DH)


def reference(x, pos, g1, g2, wq, wk, wv, wo, w1, w3, w2):
    a = rms_norm(x, g1)
    q = rope(jnp.dot(a, wq, preferred_element_type=jnp.float32).reshape(T, HQ, DH), pos).astype(jnp.bfloat16)
    k = rope(jnp.dot(a, wk, preferred_element_type=jnp.float32).reshape(T, HKV, DH), pos).astype(jnp.bfloat16)
    v = jnp.dot(a, wv, preferred_element_type=jnp.float32).astype(jnp.bfloat16).reshape(T, HKV, DH)
    o = attention(q, k, v, pos)
    h1 = (x.astype(jnp.float32) + jnp.dot(o, wo, preferred_element_type=jnp.float32)).astype(jnp.bfloat16)
    b = rms_norm(h1, g2)
    hid = (jax.nn.silu(jnp.dot(b, w1, preferred_element_type=jnp.float32)) * jnp.dot(b, w3, preferred_element_type=jnp.float32)).astype(jnp.bfloat16)
    return (h1.astype(jnp.float32) + jnp.dot(hid, w2, preferred_element_type=jnp.float32)).astype(jnp.bfloat16)
```

```python
import functools
import math

import jax
import jax.numpy as jnp
from jax import lax
from jax.experimental import pallas as pl
from jax.experimental.pallas import tpu as pltpu
from jax.sharding import PartitionSpec as P

DH = 128
EPS = 1e-5
THETA = 500000.0
NEG = -1e30


def rms_norm(v, g):
    vf = v.astype(jnp.float32)
    inv = lax.rsqrt(jnp.mean(vf * vf, axis=-1, keepdims=True) + EPS)
    return (vf * inv * g.astype(jnp.float32)).astype(jnp.bfloat16)


def tables(p):
    freq = 1.0 / (THETA ** (jnp.arange(0, DH, 2, dtype=jnp.float32) / DH))
    ang = p.astype(jnp.float32)[:, None] * freq
    c = jnp.cos(ang)
    s = jnp.sin(ang)
    return jnp.concatenate([c, c], axis=1), jnp.concatenate([-s, s], axis=1)


def dot32(a, b):
    return jnp.dot(a, b, preferred_element_type=jnp.float32)


def kv_kernel(u_ref, c_ref, s_ref, o_ref):
    kw = u_ref.shape[1] // 2
    c = c_ref[...]
    s = s_ref[...]
    for h in range(kw // DH):
        u = u_ref[:, h * DH:(h + 1) * DH]
        o_ref[:, h * DH:(h + 1) * DH] = (u * c + pltpu.roll(u, DH // 2, 1) * s).astype(jnp.bfloat16)
    o_ref[:, kw:] = u_ref[:, kw:].astype(jnp.bfloat16)


def kv_finish(u, c, s):
    return pl.pallas_call(
        kv_kernel,
        out_shape=jax.ShapeDtypeStruct(u.shape, jnp.bfloat16),
        cost_estimate=pl.CostEstimate(flops=2 * 10**9, bytes_accessed=6 * u.size, transcendentals=0),
        name="kv_finish",
    )(u, c, s)


LOW = (0, -1, 2, 1)
HIGH = (0, 1, 2, -1)


def attn_kernel(ntp, ncp, bat, info_ref, q_ref, c_ref, s_ref, *rest):
    kvs = rest[:8]
    o_ref, kv, qs, acc, ms, ls, sem = rest[8:]
    piece = q_ref.shape[0] // 2
    heads = q_ref.shape[1] // DH
    kvh = kv.shape[1] // (2 * DH)
    grp = heads // kvh
    mrow = grp * piece
    blk = ntp * piece
    npc = 2 * ntp * ncp
    cc = info_ref[0]
    jj = info_ref[1]

    copies = []
    for b in range(4):
        for side in range(2):
            src = kvs[2 * b + side]
            core = lax.rem(cc, 2)
            c0 = cc if side == 0 else cc + 1 - 2 * core
            for e, d in enumerate((0, ncp - 2, 2, 4)):
                ce = lax.rem(c0 + d, ncp)
                for half in range(2):
                    off = (LOW, HIGH)[half][b]
                    k = ce * ntp + lax.rem(jj + off + ntp, ntp)
                    p = k if half == 0 else npc - 1 - k
                    copies.append(pltpu.make_async_copy(
                        src.at[pl.ds((2 * e + half) * piece, piece), :],
                        kv.at[pl.ds(pl.multiple_of(p * piece, piece), piece), :],
                        sem))
    for c in copies:
        c.start()

    for half in range(2):
        r0 = half * piece
        c = c_ref[r0:r0 + piece, :]
        s = s_ref[r0:r0 + piece, :]
        for h in range(heads):
            u = q_ref[r0:r0 + piece, h * DH:(h + 1) * DH]
            qs[half, h // grp, (h % grp) * piece:(h % grp + 1) * piece, :] = (
                u * c + pltpu.roll(u, DH // 2, 1) * s).astype(jnp.bfloat16)

    for c in copies:
        c.wait()

    scale = math.log2(math.e) / math.sqrt(DH)
    for half in range(2):
        ms[...] = jnp.full_like(ms, NEG)
        ls[...] = jnp.zeros_like(ls)
        acc[...] = jnp.zeros_like(acc)
        k = cc * ntp + lax.rem(jj + (LOW, HIGH)[half][bat] + ntp, ntp)
        pq = k if half == 0 else npc - 1 - k
        nfull = cc if half == 0 else 2 * ncp - 1 - cc

        def step(i, masked, half=half, pq=pq):
            k0 = pl.multiple_of(i * blk, blk)
            for g in range(kvh):
                kk = kv[pl.ds(k0, blk), g * DH:(g + 1) * DH]
                vv = kv[pl.ds(k0, blk), (kvh + g) * DH:(kvh + g + 1) * DH]
                s = lax.dot_general(qs[half, g], kk, (((1,), (1,)), ((), ())),
                                    preferred_element_type=jnp.float32)
                if masked:
                    row = lax.broadcasted_iota(jnp.int32, (mrow, blk), 0)
                    row = lax.rem(row, piece) + pq * piece
                    col = lax.broadcasted_iota(jnp.int32, (mrow, blk), 1) + k0
                    s = jnp.where(col <= row, s, NEG)
                m_old = ms[g]
                m_new = jnp.maximum(m_old, jnp.max(s, axis=1, keepdims=True))
                alpha = jnp.exp2((m_old - m_new) * scale)
                ms[g] = m_new
                ps = []
                lsum = ls[g] * alpha
                for t in range(blk // DH):
                    pt = jnp.exp2((s[:, t * DH:(t + 1) * DH] - m_new) * scale)
                    lsum = lsum + pt
                    ps.append(pt.astype(jnp.bfloat16))
                ls[g] = lsum
                pv = jnp.dot(jnp.concatenate(ps, axis=1), vv, preferred_element_type=jnp.float32)
                acc[g] = acc[g] * alpha + pv

        lax.fori_loop(0, nfull, lambda i, z: (step(i, False), z)[1], 0)
        step(nfull, True)
        for g in range(kvh):
            o = acc[g] / jnp.sum(ls[g], axis=1, keepdims=True)
            for h in range(grp):
                hh = g * grp + h
                o_ref[half * piece:(half + 1) * piece, hh * DH:(hh + 1) * DH] = (
                    o[h * piece:(h + 1) * piece, :].astype(jnp.bfloat16))


def attend(bat, ntp, ncp, info, q, c, s, kvs):
    rows, width = q.shape
    piece = rows // 2
    kvw = kvs[0].shape[1]
    kvh = kvw // (2 * DH)
    mrow = (width // DH // kvh) * piece
    total = 2 * ntp * ncp * piece
    vm = pl.BlockSpec(memory_space=pltpu.VMEM)
    return pl.pallas_call(
        functools.partial(attn_kernel, ntp, ncp, bat),
        out_shape=jax.ShapeDtypeStruct((rows, width), jnp.bfloat16),
        in_specs=[pl.BlockSpec(memory_space=pltpu.SMEM), vm, vm, vm] + [pl.BlockSpec(memory_space=pltpu.HBM)] * 8,
        out_specs=vm,
        scratch_shapes=[
            pltpu.VMEM((total, kvw), jnp.bfloat16),
            pltpu.VMEM((2, kvh, mrow, DH), jnp.bfloat16),
            pltpu.VMEM((kvh, mrow, DH), jnp.float32),
            pltpu.VMEM((kvh, mrow, DH), jnp.float32),
            pltpu.VMEM((kvh, mrow, DH), jnp.float32),
            pltpu.SemaphoreType.DMA,
        ],
        compiler_params=pltpu.CompilerParams(vmem_limit_bytes=40 * 2**20),
        cost_estimate=pl.CostEstimate(
            flops=2 * 10**10, bytes_accessed=2 * total * kvw + 6 * q.size, transcendentals=rows * width // DH * total // 2),
    )(info, q, c, s, *kvs)


def solution(mesh):
    tok = P(('dp', 'cp', 'tp'), None)
    col = P(None, 'tp')
    row = P('tp', None)
    ntp = mesh.shape['tp']
    ncp = mesh.shape['cp']
    assert ntp == 4 and ncp == 8

    def tshift(v, d):
        return lax.ppermute(v, 'tp', [(i, (i + d) % ntp) for i in range(ntp)])

    def cshift(v, d):
        return lax.ppermute(v, 'cp', [(i, (i + d) % ncp) for i in range(ncp)])

    def cswap(v):
        return lax.ppermute(v, 'cp', [(i, i ^ 1) for i in range(ncp)])

    def cat(u, v):
        return jnp.concatenate([u, v], axis=0)

    def gather(lo, hi):
        p_lo = tshift(lo, 1)
        m_hi = tshift(hi, -1)
        p_hi = tshift(hi, 1)
        m_lo = tshift(lo, -1)
        f_lo = tshift(p_lo, 1)
        f_hi = tshift(m_hi, -1)
        return (p_lo, m_hi), (f_lo, f_hi), (m_lo, p_hi)

    def layer(x, pos, g1, g2, wq, wk, wv, wo, w1, w3, w2):
        n = x.shape[0]
        h = n // 2
        pos_p = tshift(pos, 1)
        pos_m = tshift(pos, -1)
        pos_2 = tshift(pos, 2)
        info = jnp.stack([lax.axis_index('cp'), lax.axis_index('tp')]).astype(jnp.int32)

        lo = rms_norm(x[:h], g1)
        hi = rms_norm(x[h:], g1)
        parts = [(lo, hi)] + list(gather(lo, hi))
        ptab = [pos, cat(pos_p[:h], pos_m[h:]), pos_2, cat(pos_m[:h], pos_p[h:])]
        tabs = [tables(p) for p in ptab]
        wkv = jnp.concatenate([wk, wv], axis=1)

        qs, kvs = [], []
        for b in range(4):
            a = cat(*parts[b])
            kvu = dot32(a, wkv)
            kv = kv_finish(kvu, *tabs[b])
            others = [cshift(kv, 2), cshift(kv, -2), cshift(kv, 4)]
            stack = jnp.concatenate([kv] + others, axis=0)
            kvs += [stack, cswap(stack)]
            qs.append(dot32(a, wq))

        def attn(b):
            return attend(b, ntp, ncp, info, qs[b], *tabs[b], kvs)

        def scatter(part):
            y = part(1).astype(jnp.bfloat16)
            r1_lo = tshift(y[:h], -1)
            r1_hi = tshift(y[h:], 1)
            y = part(2).astype(jnp.bfloat16)
            s_lo = tshift(y[:h], 1)
            s_hi = tshift(y[h:], -1)
            y = lax.optimization_barrier(part(3))
            y_lo = (y[:h] + s_lo.astype(jnp.float32)).astype(jnp.bfloat16)
            y_hi = (y[h:] + s_hi.astype(jnp.float32)).astype(jnp.bfloat16)
            r3_lo = tshift(y_lo, 1)
            r3_hi = tshift(y_hi, -1)
            y = part(0)
            return y, (r1_lo, r1_hi), (r3_lo, r3_hi)

        def total(base, y, r1, r3, i):
            t = base.astype(jnp.float32) + y + r1[i].astype(jnp.float32) + r3[i].astype(jnp.float32)
            return t.astype(jnp.bfloat16)

        y, r1, r3 = scatter(lambda b: dot32(attn(b), wo))
        h_lo = total(x[:h], y[:h], r1, r3, 0)
        h_hi = total(x[h:], y[h:], r1, r3, 1)

        lo = rms_norm(h_lo, g2)
        hi = rms_norm(h_hi, g2)
        parts2 = [(lo, hi)] + list(gather(lo, hi))
        hid = []
        for b in range(4):
            a = cat(*parts2[b])
            hid.append((jax.nn.silu(dot32(a, w1)) * dot32(a, w3)).astype(jnp.bfloat16))
        y, r1, r3 = scatter(lambda b: dot32(hid[b], w2))
        return cat(total(h_lo, y[:h], r1, r3, 0), total(h_hi, y[h:], r1, r3, 1))

    return jax.shard_map(layer, mesh=mesh, in_specs=(tok, P(('dp', 'cp', 'tp')), P(None), P(None), col, col, col, row, col, col, row),
                         out_specs=tok, check_vma=False)
```

```python
import functools
import math

import jax
import jax.numpy as jnp
from jax import lax
from jax.experimental import pallas as pl
from jax.experimental.pallas import tpu as pltpu
from jax.sharding import PartitionSpec as P

DH = 128
EPS = 1e-5
THETA = 500000.0
NEG = -1e30


def rms_norm(v, g):
    vf = v.astype(jnp.float32)
    inv = lax.rsqrt(jnp.mean(vf * vf, axis=-1, keepdims=True) + EPS)
    return (vf * inv * g.astype(jnp.float32)).astype(jnp.bfloat16)


def tables(p):
    freq = 1.0 / (THETA ** (jnp.arange(0, DH, 2, dtype=jnp.float32) / DH))
    ang = p.astype(jnp.float32)[:, None] * freq
    c = jnp.cos(ang)
    s = jnp.sin(ang)
    return jnp.concatenate([c, c], axis=1), jnp.concatenate([-s, s], axis=1)


def dot32(a, b):
    return jnp.dot(a, b, preferred_element_type=jnp.float32)


def chunk(n, most):
    c = most
    while n % c:
        c = c // 2
    return c


def proj_kernel(roped, lo_ref, hi_ref, c_ref, s_ref, *rest):
    n = len(roped)
    ws, o_ref, acc = rest[:n], rest[n], rest[n + 1]
    i = pl.program_id(0)
    a = jnp.concatenate([lo_ref[...], hi_ref[...]], axis=0)

    @pl.when(i == 0)
    def _():
        acc[...] = jnp.zeros_like(acc)

    at = 0
    for w in ws:
        wide = w.shape[1]
        acc[:, at:at + wide] += dot32(a, w[...])
        at += wide

    @pl.when(i == pl.num_programs(0) - 1)
    def _():
        c = c_ref[...]
        s = s_ref[...]
        at = 0
        for w, rot in zip(ws, roped):
            for _ in range(w.shape[1] // DH):
                u = acc[:, at:at + DH]
                if rot:
                    u = u * c + pltpu.roll(u, DH // 2, 1) * s
                o_ref[:, at:at + DH] = u.astype(jnp.bfloat16)
                at += DH


def project(lo, hi, c, s, ws, roped):
    h, depth = lo.shape
    wide = sum(w.shape[1] for w in ws)
    kb = chunk(depth, 1024)
    tab = pl.BlockSpec((2 * h, DH), lambda i: (0, 0))
    act = pl.BlockSpec((h, kb), lambda i: (0, i))
    return pl.pallas_call(
        functools.partial(proj_kernel, roped),
        out_shape=jax.ShapeDtypeStruct((2 * h, wide), jnp.bfloat16),
        grid=(depth // kb,),
        in_specs=[act, act, tab, tab] + [pl.BlockSpec((kb, w.shape[1]), lambda i: (i, 0)) for w in ws],
        out_specs=pl.BlockSpec((2 * h, wide), lambda i: (0, 0)),
        scratch_shapes=[pltpu.VMEM((2 * h, wide), jnp.float32)],
        compiler_params=pltpu.CompilerParams(dimension_semantics=("arbitrary",)),
        cost_estimate=pl.CostEstimate(flops=4 * h * depth * wide, bytes_accessed=2 * depth * (wide + 2 * h), transcendentals=0),
    )(lo, hi, c, s, *ws)


def gate_kernel(lo_ref, hi_ref, w1_ref, w3_ref, o_ref, acc1, acc3):
    i = pl.program_id(0)
    a = jnp.concatenate([lo_ref[...], hi_ref[...]], axis=0)

    @pl.when(i == 0)
    def _():
        acc1[...] = jnp.zeros_like(acc1)
        acc3[...] = jnp.zeros_like(acc3)

    acc1[...] += dot32(a, w1_ref[...])
    acc3[...] += dot32(a, w3_ref[...])

    @pl.when(i == pl.num_programs(0) - 1)
    def _():
        o_ref[...] = (jax.nn.silu(acc1[...]) * acc3[...]).astype(jnp.bfloat16)


def gate(lo, hi, w1, w3):
    h, depth = lo.shape
    wide = w1.shape[1]
    kb = chunk(depth, 512)
    act = pl.BlockSpec((h, kb), lambda i: (0, i))
    wsp = pl.BlockSpec((kb, wide), lambda i: (i, 0))
    return pl.pallas_call(
        gate_kernel,
        out_shape=jax.ShapeDtypeStruct((2 * h, wide), jnp.bfloat16),
        grid=(depth // kb,),
        in_specs=[act, act, wsp, wsp],
        out_specs=pl.BlockSpec((2 * h, wide), lambda i: (0, 0)),
        scratch_shapes=[pltpu.VMEM((2 * h, wide), jnp.float32)] * 2,
        compiler_params=pltpu.CompilerParams(dimension_semantics=("arbitrary",)),
        cost_estimate=pl.CostEstimate(flops=8 * h * depth * wide, bytes_accessed=4 * depth * (wide + h), transcendentals=2 * h * wide),
    )(lo, hi, w1, w3)


def down_kernel(a_ref, w_ref, lo_ref, hi_ref):
    h = lo_ref.shape[0]
    y = dot32(a_ref[...], w_ref[...])
    lo_ref[...] = y[:h].astype(lo_ref.dtype)
    hi_ref[...] = y[h:].astype(hi_ref.dtype)


def down(a, w, dtype):
    rows, depth = a.shape
    wide = w.shape[1]
    nb = chunk(wide, 512)
    out = pl.BlockSpec((rows // 2, nb), lambda i: (0, i))
    return pl.pallas_call(
        down_kernel,
        out_shape=[jax.ShapeDtypeStruct((rows // 2, wide), dtype)] * 2,
        grid=(wide // nb,),
        in_specs=[pl.BlockSpec((rows, depth), lambda i: (0, 0)), pl.BlockSpec((depth, nb), lambda i: (0, i))],
        out_specs=[out, out],
        compiler_params=pltpu.CompilerParams(dimension_semantics=("arbitrary",)),
        cost_estimate=pl.CostEstimate(flops=2 * rows * depth * wide, bytes_accessed=2 * depth * (wide + rows), transcendentals=0),
    )(a, w)


LOW = (0, -1, 2, 1)
HIGH = (0, 1, 2, -1)


def attn_kernel(ntp, ncp, bat, info_ref, q_ref, *rest):
    kvs = rest[:8]
    wo_hbm, lo_ref, hi_ref, kv, wo, qs, acc, ms, ls, o, ksem, wsem = rest[8:]
    piece = q_ref.shape[0] // 2
    heads = q_ref.shape[1] // DH
    kvh = kv.shape[1] // (2 * DH)
    grp = heads // kvh
    mrow = grp * piece
    blk = ntp * piece
    npc = 2 * ntp * ncp
    cc = info_ref[0]
    jj = info_ref[1]
    mate = cc + 1 - 2 * lax.rem(cc, 2)
    last = 2 * ncp - 1 - cc

    def owner(s):
        low = s < ncp
        return jnp.where(low, s, 2 * ncp - 1 - s), jnp.where(low, 0, 1)

    def piece_of(c_src, half, b):
        kl = c_src * ntp + lax.rem(jj + LOW[b] + ntp, ntp)
        kh = c_src * ntp + lax.rem(jj + HIGH[b] + ntp, ntp)
        return jnp.where(half == 0, kl, npc - 1 - kh)

    def load(s, z):
        c_src, half = owner(s)
        same = lax.rem(c_src + cc, 2) == 0
        e = lax.rem(c_src - jnp.where(same, cc, mate) + ncp, ncp) // 2
        off = pl.multiple_of((2 * e + half) * piece, piece)
        for b in range(4):
            dst = kv.at[pl.ds(pl.multiple_of(s * blk + b * piece, piece), piece), :]

            @pl.when(same)
            def _():
                pltpu.make_async_copy(kvs[2 * b].at[pl.ds(off, piece), :], dst, ksem.at[s]).start()

            @pl.when(jnp.logical_not(same))
            def _():
                pltpu.make_async_copy(kvs[2 * b + 1].at[pl.ds(off, piece), :], dst, ksem.at[s]).start()
        return z

    lax.fori_loop(0, last + 1, load, 0)
    wcopy = pltpu.make_async_copy(wo_hbm, wo, wsem)
    wcopy.start()

    scale = math.log2(math.e) / math.sqrt(DH)

    def one_half(turn, z):
        half = 1 - turn
        r0 = pl.multiple_of(half * piece, piece)
        ms[...] = jnp.full_like(ms, NEG)
        ls[...] = jnp.zeros_like(ls)
        acc[...] = jnp.zeros_like(acc)
        for h in range(heads):
            qs[h // grp, (h % grp) * piece:(h % grp + 1) * piece, :] = q_ref[pl.ds(r0, piece), h * DH:(h + 1) * DH]
        diag = jnp.where(half == 0, cc, last)

        def step(i, masked):
            k0 = pl.multiple_of(i * blk, blk)

            @pl.when(turn == 0)
            def _():
                dst = kv.at[pl.ds(k0, blk), :]
                pltpu.make_async_copy(dst, dst, ksem.at[i]).wait()

            ss = []
            for g in range(kvh):
                kk = kv[pl.ds(k0, blk), g * DH:(g + 1) * DH]
                ss.append(lax.dot_general(qs[g], kk, (((1,), (1,)), ((), ())), preferred_element_type=jnp.float32))
            if masked:
                c_src, hf = owner(i)
                row = lax.broadcasted_iota(jnp.int32, (mrow, 1), 0)
                row = lax.rem(row, piece) + piece_of(cc, half, bat) * piece
                col = lax.broadcasted_iota(jnp.int32, (1, blk), 1)
                base = jnp.zeros((1, blk), jnp.int32)
                for b in range(4):
                    base = jnp.where(col >= b * piece, (piece_of(c_src, hf, b) - b) * piece, base)
                keep = (col + base) <= row
                ss = [jnp.where(keep, s, NEG) for s in ss]
            for g in range(kvh):
                s = ss[g]
                vv = kv[pl.ds(k0, blk), (kvh + g) * DH:(kvh + g + 1) * DH]
                m_old = ms[g]
                m_new = jnp.maximum(m_old, jnp.max(s, axis=1, keepdims=True))
                alpha = jnp.exp2((m_old - m_new) * scale)
                ms[g] = m_new
                ps = []
                lsum = ls[g] * alpha
                for t in range(blk // DH):
                    pt = jnp.exp2((s[:, t * DH:(t + 1) * DH] - m_new) * scale)
                    lsum = lsum + pt
                    ps.append(pt.astype(jnp.bfloat16))
                ls[g] = lsum
                acc[g] = acc[g] * alpha + dot32(jnp.concatenate(ps, axis=1), vv)

        lax.fori_loop(0, diag, lambda i, y: (step(i, False), y)[1], 0)
        step(diag, True)
        for g in range(kvh):
            og = acc[g] / jnp.sum(ls[g], axis=1, keepdims=True)
            for h in range(grp):
                hh = g * grp + h
                o[pl.ds(r0, piece), hh * DH:(hh + 1) * DH] = og[h * piece:(h + 1) * piece, :].astype(jnp.bfloat16)
        return z

    lax.fori_loop(0, 2, one_half, 0)
    wcopy.wait()
    nb = chunk(wo.shape[1], 512)

    def out(n, z):
        cols = pl.ds(pl.multiple_of(n * nb, nb), nb)
        y = dot32(o[...], wo[:, cols])
        lo_ref[:, cols] = y[:piece].astype(lo_ref.dtype)
        hi_ref[:, cols] = y[piece:].astype(hi_ref.dtype)
        return z

    lax.fori_loop(0, wo.shape[1] // nb, out, 0)


def attend(bat, ntp, ncp, info, q, kvs, wo, dtype):
    rows, width = q.shape
    piece = rows // 2
    kvw = kvs[0].shape[1]
    kvh = kvw // (2 * DH)
    mrow = (width // DH // kvh) * piece
    total = 2 * ntp * ncp * piece
    vm = pl.BlockSpec(memory_space=pltpu.VMEM)
    hbm = pl.BlockSpec(memory_space=pltpu.HBM)
    state = pltpu.VMEM((kvh, mrow, DH), jnp.float32)
    return pl.pallas_call(
        functools.partial(attn_kernel, ntp, ncp, bat),
        out_shape=[jax.ShapeDtypeStruct((piece, wo.shape[1]), dtype)] * 2,
        in_specs=[pl.BlockSpec(memory_space=pltpu.SMEM), vm] + [hbm] * 9,
        out_specs=[vm, vm],
        scratch_shapes=[
            pltpu.VMEM((total, kvw), jnp.bfloat16),
            pltpu.VMEM(wo.shape, jnp.bfloat16),
            pltpu.VMEM((kvh, mrow, DH), jnp.bfloat16),
            state, state, state,
            pltpu.VMEM((rows, width), jnp.bfloat16),
            pltpu.SemaphoreType.DMA((2 * ncp,)),
            pltpu.SemaphoreType.DMA,
        ],
        cost_estimate=pl.CostEstimate(
            flops=2 * 10**10, bytes_accessed=2 * total * kvw + 2 * wo.size, transcendentals=rows * width // DH * total // 2),
    )(info, q, *kvs, wo)


def solution(mesh):
    tok = P(('dp', 'cp', 'tp'), None)
    col = P(None, 'tp')
    row = P('tp', None)
    ntp = mesh.shape['tp']
    ncp = mesh.shape['cp']
    assert ntp == 4 and ncp == 8

    def tshift(v, d):
        return lax.ppermute(v, 'tp', [(i, (i + d) % ntp) for i in range(ntp)])

    def cshift(v, d):
        return lax.ppermute(v, 'cp', [(i, (i + d) % ncp) for i in range(ncp)])

    def cswap(v):
        return lax.ppermute(v, 'cp', [(i, i ^ 1) for i in range(ncp)])

    def cat(u, v):
        return jnp.concatenate([u, v], axis=0)

    def gather(lo, hi):
        p_lo = tshift(lo, 1)
        m_hi = tshift(hi, -1)
        p_hi = tshift(hi, 1)
        m_lo = tshift(lo, -1)
        f_lo = tshift(p_lo, 1)
        f_hi = tshift(m_hi, -1)
        return (p_lo, m_hi), (f_lo, f_hi), (m_lo, p_hi)

    def layer(x, pos, g1, g2, wq, wk, wv, wo, w1, w3, w2):
        n = x.shape[0]
        h = n // 2
        pos_p = tshift(pos, 1)
        pos_m = tshift(pos, -1)
        pos_2 = tshift(pos, 2)
        info = jnp.stack([lax.axis_index('cp'), lax.axis_index('tp')]).astype(jnp.int32)

        lo = rms_norm(x[:h], g1)
        hi = rms_norm(x[h:], g1)
        parts = [(lo, hi)] + list(gather(lo, hi))
        ptab = [pos, cat(pos_p[:h], pos_m[h:]), pos_2, cat(pos_m[:h], pos_p[h:])]
        tabs = [tables(p) for p in ptab]
        qs, kvs = [], []
        for b in range(4):
            kv = project(*parts[b], *tabs[b], (wk, wv), (True, False))
            stack = jnp.concatenate([kv, cshift(kv, -2), cshift(kv, 4), cshift(kv, 2)], axis=0)
            kvs += [stack, cswap(stack)]
            qs.append(project(*parts[b], *tabs[b], (wq,), (True,)))

        def scatter(part):
            y_lo, y_hi = part(1, jnp.bfloat16)
            r1_lo = tshift(y_lo, -1)
            r1_hi = tshift(y_hi, 1)
            y_lo, y_hi = part(2, jnp.bfloat16)
            s_lo = tshift(y_lo, 1)
            s_hi = tshift(y_hi, -1)
            y_lo, y_hi = part(3, jnp.float32)
            y_lo = (y_lo + s_lo.astype(jnp.float32)).astype(jnp.bfloat16)
            y_hi = (y_hi + s_hi.astype(jnp.float32)).astype(jnp.bfloat16)
            r3_lo = tshift(y_lo, 1)
            r3_hi = tshift(y_hi, -1)
            return part(0, jnp.float32), (r1_lo, r1_hi), (r3_lo, r3_hi)

        def total(base, y, r1, r3, i):
            t = base.astype(jnp.float32) + y + r1[i].astype(jnp.float32) + r3[i].astype(jnp.float32)
            return t.astype(jnp.bfloat16)

        y, r1, r3 = scatter(lambda b, t: attend(b, ntp, ncp, info, qs[b], kvs, wo, t))
        h_lo = total(x[:h], y[0], r1, r3, 0)
        h_hi = total(x[h:], y[1], r1, r3, 1)

        lo = rms_norm(h_lo, g2)
        hi = rms_norm(h_hi, g2)
        parts2 = [(lo, hi)] + list(gather(lo, hi))
        hid = []
        for b in range(4):
            hid.append(gate(*parts2[b], w1, w3))

        def part(b, t):
            return down(hid[b], w2, t)

        y, r1, r3 = scatter(part)
        return cat(total(h_lo, y[0], r1, r3, 0), total(h_hi, y[1], r1, r3, 1))

    return jax.shard_map(layer, mesh=mesh, in_specs=(tok, P(('dp', 'cp', 'tp')), P(None), P(None), col, col, col, row, col, col, row),
                         out_specs=tok, check_vma=False)
```
